32 devices in a mesh: dp: 8 (over y, x, core), rep: 4 (over z).
Axes of the slice: x: 2, y: 2, z: 4, core: 2. Of those that a mesh axis runs over, the one named last changes fastest.
Arguments:
- tokens: bfloat16 [4096, 2048], P(('dp', 'rep')), may hold values from -6 to 6
- cotangent: bfloat16 [4096, 2048], P(('dp', 'rep')), may hold values from -0.125 to 0.125
- doc_ids: int32 [64, 64], P(('dp', 'rep')), may hold values from 0 to 3, never falling along the last dimension, each value on 1 to 32 neighbouring positions
- valid_len: int32 [64], P(('dp', 'rep')), may hold values from 16 to 64
- w_qkv: bfloat16 [2048, 384], P('dp'), may hold values from -0.125 to 0.125
- w_out: bfloat16 [2048, 128], P('dp'), may hold values from -0.5 to 0.5
- norm_gain: bfloat16 [2048], P('dp'), may hold values from 0.5 to 1.5
Outputs:
- grad_qkv: float32 [2048, 384], P('dp')
- grad_out: float32 [2048, 128], P('dp')
- grad_gain: float32 [2048], P('dp')
The draws below stay inside these ranges and needn't reach their ends.
Inputs may be any that keep to these rules, and one draw needn't show every extreme that they name: `doc_ids`: within each row of 64 positions the ids never fall, and a document has 1 to 32 positions.
All inputs are finite; a program needn't handle non-finite values.
Results may differ from the reference program's by a relative error of at most 0.0079.
Values may be sent and summed in bfloat16 or wider, within the bound.
No kernel may reach another device: no remote copies, remote signals or barrier semaphores. Data moves between devices by JAX's collectives and lax.ppermute only.
A program may use at most 64 MiB of HBM per device.

```python
import math
import jax
import jax.numpy as jnp
import numpy as np
from jax import lax

D = 2048
HD = 128
SEQ = 64
DOCS = 4
SAMPLES = 64
TOKENS = 4096
N_REP = 4


def touch_ends(entries, rng, least, largest):
    shape = entries.shape
    place = [jax.random.randint(jax.random.fold_in(rng, axis), (), 0, shape[axis]) for axis in range(len(shape))]
    entries = entries.at[tuple(place)].set(least)
    longest = shape.index(max(shape))
    place[longest] = (place[longest] + 1) % shape[longest]
    return entries.at[tuple(place)].set(largest)


def with_spikes(values, rng, source, target, blocks, factor):
    def block_of(dim):
        return (jnp.arange(values.shape[dim]) // (values.shape[dim] // blocks)).reshape((-1,) + (1,) * (values.ndim - 1 - dim))

    first = jax.random.permutation(rng, blocks)[block_of(target)]
    far = (block_of(target) + blocks // 2) % blocks
    return jnp.where((block_of(source) == first) | (block_of(source) == far), factor * values, values)


def shard_levels(stream_key, extent, split, low, top_value):
    def one(position, parts):
        heights = jax.random.uniform(jax.random.fold_in(jax.random.fold_in(stream_key, 6), position), (parts,), jnp.float32, low / len(split), top_value / len(split))
        return jnp.repeat(jnp.exp(heights), extent[position] // parts).reshape((-1,) + (1,) * (len(extent) - position - 1))

    factor_of = one(*split[0])
    for cut in split[1:]:
        factor_of = factor_of * one(*cut)
    return factor_of


def split_up(count, total, reach, skew):
    loads = [(1 << 20) // math.isqrt(standing ** skew) + 1 for standing in range(2, count + 1)]
    surplus, counts = total - reach - (count - 1), [1] * (count - 1)
    while surplus > 0:
        free = [i for i in range(count - 1) if counts[i] < reach]
        pool, remaining = sum([loads[i] for i in free]), surplus
        for i in free:
            addition = min(reach - counts[i], max(1, remaining * loads[i] // pool), surplus)
            counts[i] = counts[i] + addition
            surplus = surplus - addition
    return np.array([reach] + counts)


def ragged_sizes(key, count, total, reach, skew):
    if count == 2:
        one = jax.random.randint(key, (), max(1, total - reach), min(reach, total - 1) + 1)
        return jnp.stack([one, total - one])
    lengths = jnp.asarray(split_up(count, total, reach, skew), jnp.int32)
    twos = (count - 1) // 2
    donor, taker = lengths[1:1 + 2 * twos:2], lengths[2:2 + 2 * twos:2]
    room = jnp.minimum(donor - 1, reach - taker)
    moved = jax.random.randint(jax.random.fold_in(key, 1), (twos,), 0, 1 << 20) % (room + 1)
    lengths = lengths.at[1:1 + 2 * twos:2].set(donor - moved).at[2:2 + 2 * twos:2].set(taker + moved)
    return lengths[jax.random.permutation(jax.random.fold_in(key, 2), count)]


def centred(rng, dims, deviation, most, split=(), kind=jnp.bfloat16):
    level = shard_levels(rng, dims, split, -0.22, 0.18) if split else 1.0
    array = jax.random.normal(rng, dims, jnp.float32) * deviation * level
    return jnp.minimum(jnp.maximum(array, -most), most).astype(kind)


def gaussian_with(own_key, shape, width, most, pieces, heavy, kind=jnp.bfloat16):
    values = width * jax.random.normal(own_key, shape, jnp.float32)
    if pieces:
        values = values * shard_levels(own_key, shape, pieces, -0.22, 0.18)
    return jnp.clip(with_spikes(values, jax.random.fold_in(own_key, 3), *heavy), -most, most).astype(kind)


def setup_inputs(seed: int = 0) -> dict:
    arg_keys = jax.random.split(jax.random.key(seed), 8)
    return {
        "tokens": gaussian_with(arg_keys[0], (TOKENS, D), 1.0, 6.0, ((0, 32),), (0, 1, 32, 2.75)),
        "cotangent": gaussian_with(arg_keys[1], (TOKENS, D), 0.01, 0.125, ((0, 32),), (0, 1, 32, 2.75)),
        "doc_ids": jax.vmap(lambda own: jnp.searchsorted(jnp.cumsum(ragged_sizes(own, DOCS, SEQ, SEQ // 2, 0)), jnp.arange(SEQ), side="right"))(jax.random.split(arg_keys[2], SAMPLES)).reshape((SAMPLES, SEQ)).astype(jnp.int32),
        "valid_len": touch_ends(jax.random.randint(arg_keys[3], (SAMPLES,), SEQ // 4, SEQ + 1), jax.random.fold_in(arg_keys[3], 1), SEQ // 4, SEQ).astype(jnp.int32),
        "w_qkv": centred(arg_keys[4], (D, 3 * HD), D ** -0.5, 0.125, ((0, 8),)),
        "w_out": centred(arg_keys[5], (D, HD), HD ** -0.5, 0.5, ((0, 8),)),
        "norm_gain": jnp.clip(1.0 + 0.1 * jax.random.normal(arg_keys[6], (D,), jnp.float32), 0.5, 1.5).astype(jnp.bfloat16),
    }


NORM_EPS = 1e-06
ROPE_BASE = 1000000.0

def rotate(vector):
    half_size = vector.shape[-1] // 2
    return jnp.concatenate([-vector[..., half_size:], vector[..., :half_size]], axis=-1)

def unrotate(vector):
    half_size = vector.shape[-1] // 2
    return jnp.concatenate([vector[..., half_size:], -vector[..., :half_size]], axis=-1)

def tables(doc_rows, head_size):
    seq_length = doc_rows.shape[1]
    earlier = lax.optimization_barrier(jnp.sum((doc_rows[:, None, :] < doc_rows[:, :, None]).astype(jnp.int32), axis=2))
    offsets = (jnp.arange(seq_length, dtype=jnp.int32)[None, :] - earlier).astype(jnp.float32)
    frequency = ROPE_BASE ** (-2.0 * jnp.arange(head_size // 2, dtype=jnp.float32) / head_size)
    angles = offsets[:, :, None] * frequency
    angles = jnp.concatenate([angles, angles], axis=2)
    return (jnp.cos(angles), jnp.sin(angles))

def reference(tokens, cotangent, doc_ids, valid_len, w_qkv, w_out, norm_gain):
    samples, seq_length = doc_ids.shape
    model_width = tokens.shape[1]
    inputs = tokens.reshape(samples, seq_length, model_width)
    grads_in = cotangent.reshape(samples, seq_length, model_width)
    scale = 1.0 / math.sqrt(HD)
    order_row = jnp.arange(seq_length, dtype=jnp.int32)[:, None]
    order_col = jnp.arange(seq_length, dtype=jnp.int32)[None, :]

    def step(totals, item):
        x_rows, dy_rows, doc_row, valid = item
        wide_in = x_rows.astype(jnp.float32)
        inverse_rms = lax.rsqrt(lax.optimization_barrier(jnp.mean(wide_in * wide_in, axis=1, keepdims=True)) + NORM_EPS)
        scaled_in = wide_in * inverse_rms
        normed = (scaled_in * norm_gain.astype(jnp.float32)).astype(jnp.bfloat16)
        projected = jnp.dot(normed, w_qkv, preferred_element_type=jnp.float32)
        cosine, sine_part = tables(doc_row[None, :], HD)
        cosine = cosine[0]
        sine_part = sine_part[0]
        queries = projected[:, :HD]
        keys_raw = projected[:, HD:2 * HD]
        values_raw = projected[:, 2 * HD:]
        query_rot = ((queries * cosine + rotate(queries) * sine_part) * scale).astype(jnp.bfloat16)
        key_rot = (keys_raw * cosine + rotate(keys_raw) * sine_part).astype(jnp.bfloat16)
        values = values_raw.astype(jnp.bfloat16)
        scores = jnp.dot(query_rot, key_rot.T, preferred_element_type=jnp.float32)
        allowed = (doc_row[:, None] == doc_row[None, :]) & (order_col <= order_row)
        raised = jnp.where(allowed, jnp.exp(scores), 0.0)
        probabilities = raised / lax.optimization_barrier(jnp.sum(raised, axis=1, keepdims=True))
        probs_low = probabilities.astype(jnp.bfloat16)
        attended = jnp.dot(probs_low, values, preferred_element_type=jnp.float32).astype(jnp.bfloat16)
        live_rows = jnp.arange(seq_length, dtype=jnp.int32) < valid
        live_dy = jnp.where(live_rows[:, None], dy_rows, jnp.zeros((), jnp.bfloat16))
        d_attended = jnp.dot(live_dy, w_out, preferred_element_type=jnp.float32).astype(jnp.bfloat16)
        d_probs = jnp.dot(d_attended, values.T, preferred_element_type=jnp.float32)
        d_values = jnp.dot(probs_low.T, d_attended, preferred_element_type=jnp.float32)
        d_scores = (probabilities * (d_probs - lax.optimization_barrier(jnp.sum(probabilities * d_probs, axis=1, keepdims=True)))).astype(jnp.bfloat16)
        d_query = jnp.dot(d_scores, key_rot, preferred_element_type=jnp.float32) * scale
        d_key = jnp.dot(d_scores.T, query_rot, preferred_element_type=jnp.float32)
        d_query = d_query * cosine + unrotate(d_query * sine_part)
        d_key = d_key * cosine + unrotate(d_key * sine_part)
        d_qkv = jnp.concatenate([d_query, d_key, d_values], axis=1).astype(jnp.bfloat16)
        d_normed = jnp.dot(d_qkv, w_qkv.T, preferred_element_type=jnp.float32)
        gain_term = lax.optimization_barrier(jnp.sum(d_normed * scaled_in, axis=0))
        new_totals = (totals[0] + jnp.dot(normed.T, d_qkv, preferred_element_type=jnp.float32), totals[1] + jnp.dot(live_dy.T, attended, preferred_element_type=jnp.float32), totals[2] + gain_term)
        return (new_totals, None)
    initial = (jnp.zeros((model_width, 3 * HD), jnp.float32), jnp.zeros((model_width, HD), jnp.float32), jnp.zeros((model_width,), jnp.float32))
    totals, _ = lax.scan(step, initial, (inputs, grads_in, doc_ids, valid_len))
    return (totals[0] / N_REP, totals[1] / N_REP, totals[2] / N_REP)
```

```python
import math

import jax
import jax.numpy as jnp
from jax import lax
from jax.sharding import PartitionSpec as P

NORM_EPS = 1e-06
ROPE_BASE = 1000000.0


def rotate(vector):
    half_size = vector.shape[-1] // 2
    return jnp.concatenate([-vector[..., half_size:], vector[..., :half_size]], axis=-1)


def unrotate(vector):
    half_size = vector.shape[-1] // 2
    return jnp.concatenate([vector[..., half_size:], -vector[..., :half_size]], axis=-1)


def tables(doc_rows, head_size):
    seq_length = doc_rows.shape[1]
    earlier = jnp.sum((doc_rows[:, None, :] < doc_rows[:, :, None]).astype(jnp.int32), axis=2)
    offsets = (jnp.arange(seq_length, dtype=jnp.int32)[None, :] - earlier).astype(jnp.float32)
    frequency = ROPE_BASE ** (-2.0 * jnp.arange(head_size // 2, dtype=jnp.float32) / head_size)
    angles = offsets[:, :, None] * frequency
    angles = jnp.concatenate([angles, angles], axis=2)
    return (jnp.cos(angles), jnp.sin(angles))


def forward_pass(inputs, doc_rows, w_qkv_full, gain_full):
    batches, seq_length, model_width = inputs.shape
    head_size = w_qkv_full.shape[1] // 3
    scale = 1.0 / math.sqrt(head_size)
    wide_in = inputs.astype(jnp.float32)
    inverse_rms = lax.rsqrt(jnp.mean(wide_in * wide_in, axis=2, keepdims=True) + NORM_EPS)
    scaled_in = wide_in * inverse_rms
    normed = (scaled_in * gain_full.astype(jnp.float32)).astype(jnp.bfloat16)
    projected = jnp.dot(
        normed.reshape(-1, model_width), w_qkv_full, preferred_element_type=jnp.float32
    )
    projected = projected.reshape(batches, seq_length, 3 * head_size)
    cosine, sine_part = tables(doc_rows, head_size)
    queries = projected[:, :, :head_size]
    keys_raw = projected[:, :, head_size : 2 * head_size]
    values_raw = projected[:, :, 2 * head_size :]
    query_rot = ((queries * cosine + rotate(queries) * sine_part) * scale).astype(jnp.bfloat16)
    key_rot = (keys_raw * cosine + rotate(keys_raw) * sine_part).astype(jnp.bfloat16)
    values = values_raw.astype(jnp.bfloat16)
    scores = jnp.einsum("msh,mth->mst", query_rot, key_rot, preferred_element_type=jnp.float32)
    order_row = jnp.arange(seq_length, dtype=jnp.int32)[:, None]
    order_col = jnp.arange(seq_length, dtype=jnp.int32)[None, :]
    allowed = (doc_rows[:, :, None] == doc_rows[:, None, :]) & (order_col <= order_row)[None]
    raised = jnp.where(allowed, jnp.exp(scores), 0.0)
    probabilities = raised / jnp.sum(raised, axis=2, keepdims=True)
    probs_low = probabilities.astype(jnp.bfloat16)
    attended = jnp.einsum(
        "mst,mth->msh", probs_low, values, preferred_element_type=jnp.float32
    ).astype(jnp.bfloat16)
    return (
        scaled_in,
        normed,
        query_rot,
        key_rot,
        values,
        probabilities,
        probs_low,
        attended,
        cosine,
        sine_part,
    )


def backward_pass(saved, live_dy, w_qkv_full, w_out_full):
    (
        scaled_in,
        normed,
        query_rot,
        key_rot,
        values,
        probabilities,
        probs_low,
        attended,
        cosine,
        sine_part,
    ) = saved
    batches, seq_length, model_width = live_dy.shape
    head_size = w_out_full.shape[1]
    scale = 1.0 / math.sqrt(head_size)
    d_attended = jnp.dot(
        live_dy.reshape(-1, model_width), w_out_full, preferred_element_type=jnp.float32
    )
    d_attended = d_attended.reshape(batches, seq_length, head_size).astype(jnp.bfloat16)
    d_probs = jnp.einsum("msh,mth->mst", d_attended, values, preferred_element_type=jnp.float32)
    d_values = jnp.einsum("mst,msh->mth", probs_low, d_attended, preferred_element_type=jnp.float32)
    d_scores = (
        probabilities * (d_probs - jnp.sum(probabilities * d_probs, axis=2, keepdims=True))
    ).astype(jnp.bfloat16)
    d_query = (
        jnp.einsum("mst,mth->msh", d_scores, key_rot, preferred_element_type=jnp.float32) * scale
    )
    d_key = jnp.einsum("mst,msh->mth", d_scores, query_rot, preferred_element_type=jnp.float32)
    d_query = d_query * cosine + unrotate(d_query * sine_part)
    d_key = d_key * cosine + unrotate(d_key * sine_part)
    d_qkv = jnp.concatenate([d_query, d_key, d_values], axis=2).astype(jnp.bfloat16)
    d_normed = lax.dot_general(
        d_qkv.reshape(-1, 3 * head_size),
        w_qkv_full,
        (((1,), (1,)), ((), ())),
        preferred_element_type=jnp.float32,
    )
    gain_term = jnp.sum(d_normed * scaled_in.reshape(-1, model_width), axis=0)
    return (d_qkv, gain_term)


def shards(tokens, cotangent, doc_ids, valid_len, w_qkv, w_out, norm_gain):
    batches, seq_length = doc_ids.shape
    model_width = tokens.shape[1]
    inputs = tokens.reshape(batches, seq_length, model_width)
    live_rows = jnp.arange(seq_length, dtype=jnp.int32)[None, :] < valid_len[:, None]
    live_dy = jnp.where(
        live_rows[:, :, None],
        cotangent.reshape(batches, seq_length, model_width),
        jnp.zeros((), jnp.bfloat16),
    )
    full_set = (
        lax.all_gather(w_qkv, "dp", axis=0, tiled=True),
        lax.all_gather(w_out, "dp", axis=0, tiled=True),
        lax.all_gather(norm_gain, "dp", axis=0, tiled=True),
    )
    saved = forward_pass(inputs, doc_ids, full_set[0], full_set[2])
    qkv_all, gain_total = backward_pass(saved, live_dy, full_set[0], full_set[1])
    normed_all = saved[1]
    attended_all = saved[7]
    head_size = w_out.shape[1]
    normed_flat = normed_all.reshape(-1, model_width)
    qkv_flat = qkv_all.reshape(-1, 3 * head_size)
    attended_flat = attended_all.reshape(-1, head_size)
    grad_qkv = lax.dot_general(
        normed_flat, qkv_flat, (((0,), (0,)), ((), ())), preferred_element_type=jnp.float32
    )
    grad_out = lax.dot_general(
        live_dy.reshape(-1, model_width),
        attended_flat,
        (((0,), (0,)), ((), ())),
        preferred_element_type=jnp.float32,
    )
    shares = (
        lax.psum_scatter(grad_qkv, "dp", scatter_dimension=0, tiled=True),
        lax.psum_scatter(grad_out, "dp", scatter_dimension=0, tiled=True),
    )
    shares = lax.psum((shares[0], shares[1]), "rep")
    gain_whole = lax.psum(gain_total, ("dp", "rep"))
    owned_rows = w_qkv.shape[0]
    gain_start = lax.axis_index("dp") * owned_rows
    gain_owned = lax.dynamic_slice_in_dim(gain_whole, gain_start, owned_rows, 0)
    replicas = lax.axis_size("rep")
    return (shares[0] / replicas, shares[1] / replicas, gain_owned / replicas)


def xor_send(value, axis, mask):
    size = lax.axis_size(axis)
    return lax.ppermute(value, axis, [(place, place ^ mask) for place in range(size)])


def attention_grads(projected, d_attended, doc_rows, live_rows):
    batches, seq_length = doc_rows.shape
    head_size = d_attended.shape[-1]
    scale = 1.0 / math.sqrt(head_size)
    projected = projected.reshape(batches, seq_length, 3 * head_size)
    d_attended = d_attended.reshape(batches, seq_length, head_size)
    d_attended = jnp.where(live_rows[:, :, None], d_attended, 0.0).astype(jnp.bfloat16)
    cosine, sine_part = tables(doc_rows, head_size)
    queries = projected[:, :, :head_size]
    keys_raw = projected[:, :, head_size : 2 * head_size]
    values = projected[:, :, 2 * head_size :].astype(jnp.bfloat16)
    query_rot = ((queries * cosine + rotate(queries) * sine_part) * scale).astype(jnp.bfloat16)
    key_rot = (keys_raw * cosine + rotate(keys_raw) * sine_part).astype(jnp.bfloat16)
    scores = jnp.einsum("msh,mth->mst", query_rot, key_rot, preferred_element_type=jnp.float32)
    order_row = jnp.arange(seq_length, dtype=jnp.int32)[:, None]
    order_col = jnp.arange(seq_length, dtype=jnp.int32)[None, :]
    allowed = (doc_rows[:, :, None] == doc_rows[:, None, :]) & (order_col <= order_row)[None]
    raised = jnp.where(allowed, jnp.exp(scores), 0.0)
    probabilities = raised / jnp.sum(raised, axis=2, keepdims=True)
    probs_low = probabilities.astype(jnp.bfloat16)
    attended = jnp.einsum("mst,mth->msh", probs_low, values, preferred_element_type=jnp.float32)
    attended = jnp.where(live_rows[:, :, None], attended, 0.0).astype(jnp.bfloat16)
    d_probs = jnp.einsum("msh,mth->mst", d_attended, values, preferred_element_type=jnp.float32)
    d_values = jnp.einsum("mst,msh->mth", probs_low, d_attended, preferred_element_type=jnp.float32)
    d_scores = (
        probabilities * (d_probs - jnp.sum(probabilities * d_probs, axis=2, keepdims=True))
    ).astype(jnp.bfloat16)
    d_query = (
        jnp.einsum("mst,mth->msh", d_scores, key_rot, preferred_element_type=jnp.float32) * scale
    )
    d_key = jnp.einsum("mst,msh->mth", d_scores, query_rot, preferred_element_type=jnp.float32)
    d_query = d_query * cosine + unrotate(d_query * sine_part)
    d_key = d_key * cosine + unrotate(d_key * sine_part)
    d_qkv = jnp.concatenate([d_query, d_key, d_values], axis=2)
    return d_qkv.reshape(-1, 3 * head_size), attended.reshape(-1, head_size)


def sum_over(axis, parts):
    size = lax.axis_size(axis)
    masks = [(2 << step) - 1 for step in range(size.bit_length() - 1)]
    for step in range(len(masks)):
        low = [part.astype(jnp.bfloat16) for part in parts]
        other = [
            xor_send(part, axis, masks[(step + place) % len(masks)]) for place, part in enumerate(low)
        ]
        parts = [
            mine.astype(jnp.float32) + theirs.astype(jnp.float32)
            for mine, theirs in zip(low, other)
        ]
    return parts


def exchange_shards(tokens, cotangent, doc_ids, valid_len, w_qkv, w_out, norm_gain):
    batches, seq_length = doc_ids.shape
    rows = tokens.shape[0]
    owned = w_qkv.shape[0]
    wide = w_qkv.shape[1]
    devices = lax.axis_size("dp")
    me = lax.axis_index("dp")
    peers = range(0, devices, 2)
    gain = norm_gain.astype(jnp.float32)[:, None]
    scaled = jnp.concatenate([(w_qkv.astype(jnp.float32) * gain).astype(jnp.bfloat16), w_out], axis=1)
    gathered = [scaled] + [xor_send(scaled, "dp", mask) for mask in peers[1:]]

    def columns(array, place, width):
        return lax.dynamic_slice_in_dim(array, place * width, width, 1)

    def halves(array):
        mine = jnp.concatenate([columns(array, me ^ mask, owned) for mask in peers], axis=1)
        theirs = jnp.concatenate([columns(array, me ^ mask ^ 1, owned) for mask in peers], axis=1)
        return jnp.concatenate([mine, xor_send(theirs, "dp", 1)], axis=0)

    x_half = halves(tokens)
    dy_half = halves(cotangent)
    full = jnp.concatenate(gathered, axis=0)
    partial_qkv = jnp.dot(x_half, full[:, :wide], preferred_element_type=jnp.float32)
    partial_out = jnp.dot(dy_half, full[:, wide:], preferred_element_type=jnp.float32)
    partial = jnp.concatenate([partial_qkv, partial_out], axis=1)
    summed = partial[:rows] + xor_send(partial[rows:], "dp", 1)

    wide_in = tokens.astype(jnp.float32)
    inverse_rms = lax.rsqrt(jnp.mean(wide_in * wide_in, axis=1, keepdims=True) + NORM_EPS)
    live_rows = jnp.arange(seq_length, dtype=jnp.int32)[None, :] < valid_len[:, None]
    d_qkv, attended = attention_grads(
        summed[:, :wide] * inverse_rms, summed[:, wide:], doc_ids, live_rows
    )
    grads = jnp.concatenate([(d_qkv * inverse_rms).astype(jnp.bfloat16), attended], axis=1)

    late_tokens, late_cotangent, _ = lax.optimization_barrier((tokens, cotangent, full))
    chip = me // 2
    both = 2 * owned
    total_qkv = jnp.zeros((both, wide), jnp.float32)
    total_out = jnp.zeros((both, w_out.shape[1]), jnp.float32)
    dims = (((0,), (0,)), ((), ()))
    sent = []
    for mask in peers:
        x_part = columns(late_tokens, chip ^ (mask // 2), both)
        dy_part = columns(late_cotangent, chip ^ (mask // 2), both)
        if mask:
            x_part, dy_part = xor_send(x_part, "dp", mask), xor_send(dy_part, "dp", mask)
        sent.append((x_part, dy_part))
    x_all = jnp.concatenate([part[0] for part in sent], axis=0)
    dy_all = jnp.concatenate([part[1] for part in sent], axis=0)
    grads_all = jnp.concatenate([grads] + [xor_send(grads, "dp", mask) for mask in peers[1:]], axis=0)
    total_qkv = lax.dot_general(x_all, grads_all[:, :wide], dims, preferred_element_type=jnp.float32)
    total_out = lax.dot_general(dy_all, grads_all[:, wide:], dims, preferred_element_type=jnp.float32)
    total = jnp.concatenate([total_qkv, total_out], axis=1)
    core = me % 2
    mine = lax.dynamic_slice_in_dim(total, core * owned, owned, 0)
    theirs = lax.dynamic_slice_in_dim(total, (1 - core) * owned, owned, 0)
    total = mine + xor_send(theirs, "dp", 1)
    half = owned // 2
    first, second = sum_over("rep", [total[:half], total[half:]])
    total = jnp.concatenate([first, second], axis=0) / lax.axis_size("rep")
    raw = total[:, :wide]
    grad_gain = jnp.sum(raw * w_qkv.astype(jnp.float32), axis=1)
    return (raw * gain, total[:, wide:], grad_gain)


def power_of_two(size):
    return size & (size - 1) == 0


def solution(mesh):
    small = 2 <= mesh.shape["dp"] <= 16 and power_of_two(mesh.shape["dp"])
    body = exchange_shards if small and power_of_two(mesh.shape["rep"]) else shards
    in_specs = (
        P(("dp", "rep"), None),
        P(("dp", "rep"), None),
        P(("dp", "rep"), None),
        P(("dp", "rep")),
        P("dp", None),
        P("dp", None),
        P("dp"),
    )
    out_specs = (P("dp", None), P("dp", None), P("dp"))
    return jax.shard_map(body, mesh=mesh, in_specs=in_specs, out_specs=out_specs, check_vma=False)
```
